32 devices in a mesh: data: 1 (over z), node: 4 (over y), expert: 8 (over x, core).
Axes of the slice: x: 4, y: 4, z: 1, core: 2. Of those that a mesh axis runs over, the one named last changes fastest.
The devices are a block of a 4x4x8 slice.
Arguments:
- tokens: bfloat16 [32768, 768], P(('data', 'node', 'expert'))
- expert_ids: int32 [32768, 1], P(('data', 'node', 'expert'))
- gate_weights: float32 [32768, 1], P(('data', 'node', 'expert'))
- slot_ids: int32 [32768, 1], P(('data', 'node', 'expert'))
- w_gate: bfloat16 [32, 768, 3072], P(('node', 'expert'))
- w_up: bfloat16 [32, 768, 3072], P(('node', 'expert'))
- w_down: bfloat16 [32, 3072, 768], P(('node', 'expert'))
Outputs:
- output: bfloat16 [32768, 768], P(('data', 'node', 'expert'))
All inputs are finite; a program needn't handle non-finite values.
Results may differ from the reference program's by a relative error of at most 0.001.
Values are sent between devices in bfloat16 or wider.
A program may use at most 768 MiB of HBM per device.

```python
import jax
import jax.numpy as jnp
from jax import lax

EXPERTS = 32
D = 768
FF = 3072
TOP = 1
TOKENS_DEV = 1024
GROUP = 32
CAP = 64

TOKENS = GROUP * TOKENS_DEV


def device_slots(flat_ids):
    choice_count = flat_ids.shape[0]
    sort_order = jnp.argsort(flat_ids, stable=True)
    sorted_ids = flat_ids[sort_order]
    counts = jnp.zeros((EXPERTS,), jnp.int32).at[flat_ids].add(1)
    starts = jnp.cumsum(counts) - counts
    rank_sorted = jnp.arange(choice_count, dtype=jnp.int32) - starts[sorted_ids]
    rank_all = jnp.zeros((choice_count,), jnp.int32).at[sort_order].set(rank_sorted)
    return jnp.where(rank_all < CAP, rank_all, -1)


def draw_routing(key):
    sub_keys = jax.random.split(key, 5)
    hot_first = jax.random.randint(sub_keys[0], (), 0, EXPERTS)
    pick_hot = jax.random.randint(sub_keys[1], (TOKENS,), 0, 4)
    hot_base = jax.random.randint(sub_keys[2], (TOKENS,), 0, max(EXPERTS // 4, 1))
    any_base = jax.random.randint(sub_keys[3], (TOKENS,), 0, EXPERTS)
    base_ids = jnp.where(pick_hot == 0, hot_base, any_base)
    local_row = jnp.arange(TOKENS, dtype=jnp.int32) % TOKENS_DEV
    base_ids = jnp.where(local_row < CAP, 0, base_ids)
    step_max = (EXPERTS - 1) // max(TOP - 1, 1)
    step_sizes = jax.random.randint(sub_keys[4], (TOKENS, TOP), 1, step_max + 1)
    step_sizes = step_sizes.at[:, 0].set(0)
    offsets = jnp.cumsum(step_sizes, axis=1)
    expert_ids = ((base_ids[:, None] + hot_first + offsets) % EXPERTS).astype(jnp.int32)
    slot_ids = jax.vmap(device_slots)(expert_ids.reshape(GROUP, TOKENS_DEV * TOP))
    return expert_ids, slot_ids.reshape(TOKENS, TOP).astype(jnp.int32)


def setup_inputs(seed: int = 0, part: int = 0) -> dict:
    part_key = jax.random.fold_in(jax.random.key(seed), part)
    key_tokens, key_route, key_gates = jax.random.split(part_key, 3)
    key_gate_w, key_up_w, key_down_w = jax.random.split(jax.random.key(seed + 1), 3)
    tokens = jax.random.normal(key_tokens, (TOKENS, D), jnp.float32).astype(jnp.bfloat16)
    expert_ids, slot_ids = draw_routing(key_route)
    gate_weights = (0.5 + jax.random.uniform(key_gates, (TOKENS, TOP), jnp.float32)) * TOP ** -0.5
    w_gate = (jax.random.normal(key_gate_w, (EXPERTS, D, FF), jnp.float32) * D ** -0.5).astype(jnp.bfloat16)
    w_up = (jax.random.normal(key_up_w, (EXPERTS, D, FF), jnp.float32) * D ** -0.5).astype(jnp.bfloat16)
    w_down = (jax.random.normal(key_down_w, (EXPERTS, FF, D), jnp.float32) * FF ** -0.5).astype(jnp.bfloat16)
    return {"tokens": tokens, "expert_ids": expert_ids, "gate_weights": gate_weights, "slot_ids": slot_ids, "w_gate": w_gate, "w_up": w_up, "w_down": w_down}


def expert_block(expert_rows, gate_mat, up_mat, down_mat):
    proj_gate = jnp.dot(expert_rows, gate_mat, preferred_element_type=jnp.float32)
    proj_up = jnp.dot(expert_rows, up_mat, preferred_element_type=jnp.float32)
    hidden = (jax.nn.silu(proj_gate) * proj_up).astype(jnp.bfloat16)
    return jnp.dot(hidden, down_mat, preferred_element_type=jnp.float32).astype(jnp.bfloat16)


def reference(tokens, expert_ids, gate_weights, slot_ids, w_gate, w_up, w_down):
    buffer_rows = GROUP * CAP
    source_dev = (jnp.arange(TOKENS, dtype=jnp.int32) // TOKENS_DEV)[:, None]
    kept = slot_ids >= 0
    flat_pos = jnp.where(kept, expert_ids * buffer_rows + source_dev * CAP + slot_ids, EXPERTS * buffer_rows).reshape(-1)
    tok_index = jnp.broadcast_to(jnp.arange(TOKENS, dtype=jnp.int32)[:, None], (TOKENS, TOP)).reshape(-1)
    src_table = jnp.full((EXPERTS * buffer_rows,), TOKENS, jnp.int32).at[flat_pos].set(tok_index, mode="drop")
    gate_table = jnp.zeros((EXPERTS * buffer_rows,), jnp.float32).at[flat_pos].set(gate_weights.reshape(-1), mode="drop")

    def one_expert(out_sum, operands):
        src_rows, row_gates, gate_mat, up_mat, down_mat = operands
        expert_rows = jnp.take(tokens, src_rows, axis=0, mode="fill", fill_value=0)
        expert_out = expert_block(expert_rows, gate_mat, up_mat, down_mat)
        out_sum = out_sum.at[src_rows].add(row_gates[:, None] * expert_out.astype(jnp.float32), mode="drop")
        return out_sum, None

    out_sum, _ = lax.scan(one_expert, jnp.zeros((TOKENS, D), jnp.float32), (src_table.reshape(EXPERTS, buffer_rows), gate_table.reshape(EXPERTS, buffer_rows), w_gate, w_up, w_down))
    return out_sum.astype(jnp.bfloat16)
```

```python
import functools
import random

import jax
import jax.numpy as jnp
from jax import lax
from jax.experimental import pallas as pl
from jax.experimental.pallas import tpu as pltpu
from jax.sharding import PartitionSpec as P

MESH = pl.DeviceIdType.MESH
CAP_FACTOR = 2
CORES = 2
F_CHUNK = 256
N_CHUNK = 256
GROUPS = (4, 4, 4, 4, 4, 4, 4, 4)


def capacity(rows, top_k, experts):
    return ((CAP_FACTOR * rows * top_k + 8 * experts - 1) // (8 * experts)) * 8


def partner_order(nodes, chips):
    offs = [(n, x, c) for n in range(nodes) for x in range(chips) for c in range(CORES)]
    rest = offs[1:]
    random.Random(10).shuffle(rest)
    return offs[:1] + rest


def group_plan(blocks):
    sizes = list(GROUPS) if sum(GROUPS) == blocks else [1] * blocks
    plan, first = [], 0
    for size in sizes:
        plan.append((first, size))
        first += size
    return plan


def kernel(order, nodes, chips, cap, ids_ref, slots_ref, gates_ref, tok_hbm, wg_hbm, wu_hbm, wd_hbm, out_ref,
           tok, wg, wu, wd, send, recv, hid, y, ret, acc, pos_b, gate_b,
           tok_sem, w_sem, s1, r1, s2, r2):
    rows, width = tok.shape
    ff = wg.shape[1]
    data, node, exp = lax.axis_index("data"), lax.axis_index("node"), lax.axis_index("expert")
    chip, core = exp // CORES, lax.rem(exp, CORES)

    def device(off, sign):
        dn, dx, dc = off
        n = lax.rem(node + (dn if sign > 0 else nodes - dn), nodes)
        x = lax.rem(chip + (dx if sign > 0 else chips - dx), chips)
        return n, x * CORES + lax.rem(core + dc, CORES)

    def expert_of(i):
        n, e = device(order[i], 1)
        return n * (chips * CORES) + e

    def block(i, size=1):
        return pl.ds(i * cap, size * cap)

    def dispatch(i):
        n, e = device(order[i], 1)
        return pltpu.make_async_remote_copy(send.at[block(i)], recv.at[block(i)], s1.at[i], r1.at[i],
                                            device_id=(data, n, e), device_id_type=MESH)

    def give_back(i):
        n, e = device(order[i], -1)
        return pltpu.make_async_remote_copy(y.at[block(i)], ret.at[block(i)], s2.at[i], r2.at[i],
                                            device_id=(data, n, e), device_id_type=MESH)

    blocks = len(order)
    plan = group_plan(blocks)

    tok_copy = pltpu.make_async_copy(tok_hbm, tok, tok_sem)
    tok_copy.start()
    w_copies = [pltpu.make_async_copy(h.at[0], v, w_sem.at[k]) for k, (h, v) in enumerate(((wg_hbm, wg), (wu_hbm, wu), (wd_hbm, wd)))]
    for c in w_copies:
        c.start()
    barrier = pltpu.get_barrier_semaphore()
    for i in range(1, blocks):
        n, e = device(order[i], 1)
        pl.semaphore_signal(barrier, inc=1, device_id=(data, n, e), device_id_type=MESH)

    ids, slots = ids_ref[...], slots_ref[...]
    pos = jnp.where(slots >= 0, ids * cap + slots, -1)
    tok_copy.wait()

    row_i = lax.broadcasted_iota(jnp.int32, (cap, rows), 0)

    def pick(first, size):
        hot = [jnp.where(pos - expert_of(i) * cap == row_i, 1.0, 0.0).astype(jnp.bfloat16) for i in range(first, first + size)]
        hot = jnp.concatenate(hot, axis=0)
        got = jnp.dot(hot, tok[...], preferred_element_type=jnp.float32).astype(jnp.bfloat16)
        if first == 0:
            recv[block(0)] = got[:cap]
        send[block(first, size)] = got

    def start_dispatch(first, size):
        for i in range(max(first, 1), first + size):
            dispatch(i).start()

    for k, (first, size) in enumerate(plan):
        pick(first, size)
        if k == 1:
            pl.semaphore_wait(barrier, blocks - 1)
        if k >= 1:
            start_dispatch(*plan[k - 1])
    start_dispatch(*plan[-1])

    lanes = 128
    for b in range(rows // lanes):
        part = pl.ds(b * lanes, lanes)
        pos_b[part, :] = jnp.transpose(jnp.broadcast_to(pos[:, b * lanes:(b + 1) * lanes], (lanes, lanes)))
        gate_b[part, :] = jnp.transpose(jnp.broadcast_to(gates_ref[:, b * lanes:(b + 1) * lanes], (lanes, lanes)))

    def expert_rows(first, size):
        m = size * cap
        x_rows = block(first, size)

        def up(f, carry):
            cols = pl.ds(pl.multiple_of(f * F_CHUNK, F_CHUNK), F_CHUNK)
            x = recv[x_rows]
            a = jnp.dot(x, wg[:, cols], preferred_element_type=jnp.float32)
            b = jnp.dot(x, wu[:, cols], preferred_element_type=jnp.float32)
            hid[pl.ds(0, m), cols] = (jax.nn.silu(a) * b).astype(jnp.bfloat16)
            return carry

        lax.fori_loop(0, ff // F_CHUNK, up, 0)

        def down(f, carry):
            cols = pl.ds(pl.multiple_of(f * N_CHUNK, N_CHUNK), N_CHUNK)
            y[x_rows, cols] = jnp.dot(hid[pl.ds(0, m), :], wd[:, cols], preferred_element_type=jnp.float32).astype(jnp.bfloat16)
            return carry

        lax.fori_loop(0, width // N_CHUNK, down, 0)

    for k, (first, size) in enumerate(plan):
        if k == 0:
            for c in w_copies:
                c.wait()
        for i in range(max(first, 1), first + size):
            dispatch(i).wait_recv()
        expert_rows(first, size)
        for i in range(max(first, 1), first + size):
            give_back(i).start()
        if first == 0:
            ret[block(0)] = y[block(0)]

    lane = lax.broadcasted_iota(jnp.int32, (1, lanes), 1)

    def picked(first, size):
        per = lanes // cap
        hots = []
        for i in range(first, first + size, per):
            want = lane + expert_of(i) * cap
            for q in range(1, per):
                want = jnp.where(lane >= q * cap, lane - q * cap + expert_of(i + q) * cap, want)
            hots.append(jnp.where(pos_b[...] == want, 1.0, 0.0).astype(jnp.bfloat16))
        hot = jnp.concatenate(hots, axis=1) if len(hots) > 1 else hots[0]
        return jnp.dot(hot, ret[block(first, size)], preferred_element_type=jnp.float32)

    for k, (first, size) in enumerate(plan):
        for i in range(max(first, 1), first + size):
            give_back(i).wait_recv()
        part = picked(first, size)
        if k == 0:
            acc[...] = part
        elif k < len(plan) - 1:
            acc[...] += part
        else:
            total = acc[...] + part
            gate = gate_b[...]
            for j in range(width // lanes):
                out_ref[:, j * lanes:(j + 1) * lanes] = (gate * total[:, j * lanes:(j + 1) * lanes]).astype(out_ref.dtype)

    for i in range(1, blocks):
        dispatch(i).wait_send()
        give_back(i).wait_send()


def solution(mesh):
    nodes, chips = mesh.shape["node"], mesh.shape["expert"] // CORES
    tok_spec = P(("data", "node", "expert"), None)
    weight_spec = P(("node", "expert"), None, None)
    order = partner_order(nodes, chips)

    def local_layer(tokens, expert_ids, gate_weights, slot_ids, w_gate, w_up, w_down):
        rows, width = tokens.shape
        ff = w_gate.shape[2]
        blocks = len(order)
        cap = capacity(rows, expert_ids.shape[1], blocks * w_gate.shape[0])
        slots = blocks * cap
        vmem, hbm = pl.BlockSpec(memory_space=pltpu.VMEM), pl.BlockSpec(memory_space=pl.ANY)
        bf16 = jnp.bfloat16
        return pl.pallas_call(
            functools.partial(kernel, order, nodes, chips, cap),
            out_shape=jax.ShapeDtypeStruct((rows, width), bf16),
            in_specs=[vmem, vmem, vmem, hbm, hbm, hbm, hbm],
            out_specs=vmem,
            scratch_shapes=[
                pltpu.VMEM((rows, width), bf16),
                pltpu.VMEM((width, ff), bf16),
                pltpu.VMEM((width, ff), bf16),
                pltpu.VMEM((ff, width), bf16),
                pltpu.VMEM((slots, width), bf16),
                pltpu.VMEM((slots, width), bf16),
                pltpu.VMEM((max(s for _, s in group_plan(blocks)) * cap, ff), bf16),
                pltpu.VMEM((slots, width), bf16),
                pltpu.VMEM((slots, width), bf16),
                pltpu.VMEM((rows, width), jnp.float32),
                pltpu.VMEM((rows, 128), jnp.int32),
                pltpu.VMEM((rows, 128), jnp.float32),
                pltpu.SemaphoreType.DMA,
                pltpu.SemaphoreType.DMA((3,)),
                pltpu.SemaphoreType.DMA((blocks,)),
                pltpu.SemaphoreType.DMA((blocks,)),
                pltpu.SemaphoreType.DMA((blocks,)),
                pltpu.SemaphoreType.DMA((blocks,)),
            ],
            compiler_params=pltpu.CompilerParams(collective_id=0, has_side_effects=True, vmem_limit_bytes=60 * 1024 * 1024),
            name="moe_exchange",
        )(expert_ids.reshape(1, rows), slot_ids.reshape(1, rows), gate_weights.reshape(1, rows), tokens, w_gate, w_up, w_down)

    return jax.shard_map(local_layer, mesh=mesh, in_specs=(tok_spec, tok_spec, tok_spec, tok_spec, weight_spec, weight_spec, weight_spec), out_specs=tok_spec, check_vma=False)
```

```python
import functools

import jax
import jax.numpy as jnp
from jax import lax
from jax.experimental import pallas as pl
from jax.experimental.pallas import tpu as pltpu
from jax.sharding import PartitionSpec as P

MESH = pl.DeviceIdType.MESH
CAP_FACTOR = 2
CORES = 2
LANES = 128
GROUP_ROWS = 256
X, Y = 0, 1


def capacity(rows, top_k, experts):
    return ((CAP_FACTOR * rows * top_k + 8 * experts - 1) // (8 * experts)) * 8


def far_first(n):
    return sorted(range(1, n), key=lambda d: -min(d, n - d))


class Plan:
    def __init__(self, nodes, chips, cap):
        self.size = {X: chips, Y: nodes}
        self.cap, self.half = cap, cap // 2
        self.msgs = [(a, d, c) for c in range(CORES) for i in range(max(nodes, chips) - 1) for a in (X, Y)
                     for d in far_first(self.size[a])[i:i + 1]]
        self.pieces = [(m, q) for m, (a, d, c) in enumerate(self.msgs) for q in far_first(self.size[1 - a])]
        self.piece_base = (2 + len(self.msgs)) * cap
        self.rows = self.piece_base + len(self.pieces) * self.half

    def direct_rows(self, m):
        return pl.ds((2 + m) * self.cap, self.cap)

    def piece_rows(self, k):
        return pl.ds(self.piece_base + k * self.half, self.half)

    def pieces_of(self, m):
        return [k for k, (mm, _) in enumerate(self.pieces) if mm == m]

    def spans(self):
        out = [(0, self.cap, (0, 0, 0), 0), (self.cap, self.cap, (0, 0, 1), 0)]
        for m, (a, d, c) in enumerate(self.msgs):
            out.append(((2 + m) * self.cap, self.cap, (0, d, c) if a == X else (d, 0, c), 0))
        for k, (m, q) in enumerate(self.pieces):
            a, d, c = self.msgs[m]
            out.append((self.piece_base + k * self.half, self.half, (q, d, c) if a == X else (d, q, c), 0 if a == X else self.half))
        return out


def kernel(plan, ids_ref, slots_ref, tok_hbm, wg_hbm, wu_hbm, wd_hbm, out_ref,
           tok, wg, wu, wd, send, stage, recv, hid, y, stage2, ret, acc, pos_b,
           tok_sem, w_sem, s_rel, r_rel, s_dir, r_dir, s_fwd, r_fwd, s_rdir, r_rdir, s_rpc, r_rpc, s_rfw, r_rfw):
    rows = tok.shape[0]
    cap, half = plan.cap, plan.half
    nodes, chips = plan.size[Y], plan.size[X]
    data, node, exp = lax.axis_index("data"), lax.axis_index("node"), lax.axis_index("expert")
    chip, core = exp // CORES, lax.rem(exp, CORES)
    n_msgs, n_pieces = len(plan.msgs), len(plan.pieces)

    def place(dn, dx, flip):
        n, x = lax.rem(node + dn % nodes, nodes), lax.rem(chip + dx % chips, chips)
        return n, x * CORES + lax.rem(core + flip, CORES)

    def hop(axis, d, flip):
        n, e = place(0, d, flip) if axis == X else place(d, 0, flip)
        return (data, n, e)

    def first_slot(offset, slot):
        n, e = place(*offset)
        return (n * (chips * CORES) + e) * cap + slot

    def remote(src, dst, s, r, to):
        return pltpu.make_async_remote_copy(src, dst, s, r, device_id=to, device_id_type=MESH)

    def relay(m):
        ks = plan.pieces_of(m)
        part = pl.ds(ks[0] * half, len(ks) * half)
        a, d, c = plan.msgs[m]
        return remote(send.at[pl.ds(plan.piece_base + ks[0] * half, len(ks) * half)], stage.at[part], s_rel.at[m], r_rel.at[m], hop(a, d, c))

    def forward(k):
        m, q = plan.pieces[k]
        return remote(stage.at[pl.ds(k * half, half)], recv.at[plan.piece_rows(k)], s_fwd.at[k], r_fwd.at[k], hop(1 - plan.msgs[m][0], q, 0))

    def direct(m, src, dst, s, r, sign):
        if m < 0:
            part, to = pl.ds(cap, cap), hop(X, 0, 1)
        else:
            a, d, c = plan.msgs[m]
            part, to = plan.direct_rows(m), hop(a, sign * d, c)
        return remote(src.at[part], dst.at[part], s.at[m + 1], r.at[m + 1], to)

    def out_direct(m):
        return direct(m, send, recv, s_dir, r_dir, 1)

    def back_direct(m):
        return direct(m, y, ret, s_rdir, r_rdir, -1)

    def back_piece(k):
        a, d, c = plan.msgs[plan.pieces[k][0]]
        return remote(y.at[plan.piece_rows(k)], stage2.at[pl.ds(k * half, half)], s_rpc.at[k], r_rpc.at[k], hop(a, -d, c))

    def back_forward(k):
        m, q = plan.pieces[k]
        return remote(stage2.at[pl.ds(k * half, half)], ret.at[plan.piece_rows(k)], s_rfw.at[k], r_rfw.at[k], hop(1 - plan.msgs[m][0], -q, 0))

    tok_copy = pltpu.make_async_copy(tok_hbm, tok, tok_sem)
    tok_copy.start()
    w_copies = [pltpu.make_async_copy(h.at[0], v, w_sem.at[i]) for i, (h, v) in enumerate(((wg_hbm, wg), (wu_hbm, wu), (wd_hbm, wd)))]
    for c in w_copies:
        c.start()
    barrier = pltpu.get_barrier_semaphore()
    near = [(X, 0, 1)] + plan.msgs
    for a, d, c in near:
        pl.semaphore_signal(barrier, inc=1, device_id=hop(a, d, c), device_id_type=MESH)

    ids, slots = ids_ref[...], slots_ref[...]
    pos = jnp.where(slots >= 0, ids * cap + slots, -1)
    spans = plan.spans()

    def pick(lo, hi):
        parts = [s for s in spans if lo <= s[0] < hi]
        hot = [jnp.where(pos - first_slot(off, slot) == lax.broadcasted_iota(jnp.int32, (size, rows), 0), 1.0, 0.0).astype(jnp.bfloat16)
               for _, size, off, slot in parts]
        got = jnp.dot(jnp.concatenate(hot, axis=0), tok[...], preferred_element_type=jnp.float32).astype(jnp.bfloat16)
        if lo == 0:
            recv[pl.ds(0, cap)] = got[:cap]
        send[pl.ds(lo, hi - lo)] = got

    tok_copy.wait()
    step = plan.piece_base, (plan.rows - plan.piece_base) // 4
    for i in range(4):
        pick(step[0] + i * step[1], step[0] + (i + 1) * step[1])
    pl.semaphore_wait(barrier, len(near))
    for m in range(n_msgs):
        relay(m).start()
    for lo in range(0, plan.piece_base, GROUP_ROWS):
        pick(lo, min(lo + GROUP_ROWS, plan.piece_base))
    for m in range(-1, n_msgs):
        out_direct(m).start()

    for b in range(rows // LANES):
        pos_b[pl.ds(b * LANES, LANES), :] = jnp.transpose(jnp.broadcast_to(pos[:, b * LANES:(b + 1) * LANES], (LANES, LANES)))

    for m in range(n_msgs):
        relay(m).wait_recv()
        for k in plan.pieces_of(m):
            forward(k).start()
    for c in w_copies:
        c.wait()

    n_groups = plan.rows // GROUP_ROWS

    def in_group(g):
        lo, hi = g * GROUP_ROWS, (g + 1) * GROUP_ROWS
        ms = [m for m in range(-1, n_msgs) if lo <= (2 + m) * cap < hi]
        ks = [k for k in range(n_pieces) if lo <= plan.piece_base + k * half < hi]
        return ms, ks

    def expert_group(g, carry):
        for j in range(n_groups):
            @pl.when(g == j)
            def _(j=j):
                ms, ks = in_group(j)
                for m in ms:
                    out_direct(m).wait_recv()
                for k in ks:
                    forward(k).wait_recv()
        at = pl.ds(pl.multiple_of(g * GROUP_ROWS, GROUP_ROWS), GROUP_ROWS)
        a = jnp.dot(recv[at], wg[...], preferred_element_type=jnp.float32)
        b = jnp.dot(recv[at], wu[...], preferred_element_type=jnp.float32)
        hid[...] = (jax.nn.silu(a) * b).astype(jnp.bfloat16)
        y[at] = jnp.dot(hid[...], wd[...], preferred_element_type=jnp.float32).astype(jnp.bfloat16)
        for j in range(n_groups):
            @pl.when(g == j)
            def _(j=j):
                ms, ks = in_group(j)
                for m in ms:
                    back_direct(m).start()
                for k in ks:
                    back_piece(k).start()
        return carry

    lax.fori_loop(0, n_groups, expert_group, 0)
    ret[pl.ds(0, cap)] = y[pl.ds(0, cap)]

    lane = lax.broadcasted_iota(jnp.int32, (1, LANES), 1)

    def picked(lo, hi):
        hots = []
        for at in range(lo, hi, LANES):
            want = None
            for first, size, off, slot in spans:
                if at <= first < at + LANES:
                    here = lane - (first - at) + first_slot(off, slot)
                    want = here if want is None else jnp.where(lane >= first - at, here, want)
            hots.append(jnp.where(pos_b[...] == want, 1.0, 0.0).astype(jnp.bfloat16))
        hot = jnp.concatenate(hots, axis=1) if len(hots) > 1 else hots[0]
        return jnp.dot(hot, ret[pl.ds(lo, hi - lo)], preferred_element_type=jnp.float32)

    split = n_pieces // 3
    for k in range(split):
        back_piece(k).wait_recv()
        back_forward(k).start()
    for m in range(-1, n_msgs):
        back_direct(m).wait_recv()
    acc[...] = picked(0, plan.piece_base)
    for k in range(split, n_pieces):
        back_piece(k).wait_recv()
        back_forward(k).start()
    cuts = [0, 16, 28, 32, n_pieces]
    for lo, hi in zip(cuts, cuts[1:]):
        for k in range(lo, hi):
            back_forward(k).wait_recv()
        part = picked(plan.piece_base + lo * half, plan.piece_base + hi * half)
        if hi < n_pieces:
            acc[...] += part
        else:
            out_ref[...] = (acc[...] + part).astype(out_ref.dtype)

    for m in range(n_msgs):
        relay(m).wait_send()
    for m in range(-1, n_msgs):
        out_direct(m).wait_send()
        back_direct(m).wait_send()
    for k in range(n_pieces):
        forward(k).wait_send()
        back_piece(k).wait_send()
        back_forward(k).wait_send()


def solution(mesh):
    nodes, chips = mesh.shape["node"], mesh.shape["expert"] // CORES
    tok_spec = P(("data", "node", "expert"), None)
    weight_spec = P(("node", "expert"), None, None)

    def local_layer(tokens, expert_ids, gate_weights, slot_ids, w_gate, w_up, w_down):
        rows, width = tokens.shape
        ff = w_gate.shape[2]
        cap = capacity(rows, expert_ids.shape[1], nodes * chips * CORES * w_gate.shape[0])
        plan = Plan(nodes, chips, cap)
        n_msgs, n_pieces = len(plan.msgs), len(plan.pieces)
        vmem, hbm = pl.BlockSpec(memory_space=pltpu.VMEM), pl.BlockSpec(memory_space=pl.ANY)
        bf16 = jnp.bfloat16
        sem = lambda n: pltpu.SemaphoreType.DMA((n,))
        picked = pl.pallas_call(
            functools.partial(kernel, plan),
            out_shape=jax.ShapeDtypeStruct((rows, width), bf16),
            in_specs=[vmem, vmem, hbm, hbm, hbm, hbm],
            out_specs=vmem,
            scratch_shapes=[
                pltpu.VMEM((rows, width), bf16),
                pltpu.VMEM((width, ff), bf16),
                pltpu.VMEM((width, ff), bf16),
                pltpu.VMEM((ff, width), bf16),
                pltpu.VMEM((plan.rows, width), bf16),
                pltpu.VMEM((n_pieces * plan.half, width), bf16),
                pltpu.VMEM((plan.rows, width), bf16),
                pltpu.VMEM((GROUP_ROWS, ff), bf16),
                pltpu.VMEM((plan.rows, width), bf16),
                pltpu.VMEM((n_pieces * plan.half, width), bf16),
                pltpu.VMEM((plan.rows, width), bf16),
                pltpu.VMEM((rows, width), jnp.float32),
                pltpu.VMEM((rows, LANES), jnp.int32),
                pltpu.SemaphoreType.DMA,
                sem(3), sem(n_msgs), sem(n_msgs), sem(n_msgs + 1), sem(n_msgs + 1), sem(n_pieces), sem(n_pieces),
                sem(n_msgs + 1), sem(n_msgs + 1), sem(n_pieces), sem(n_pieces), sem(n_pieces), sem(n_pieces),
            ],
            compiler_params=pltpu.CompilerParams(collective_id=0, has_side_effects=True, vmem_limit_bytes=60 * 1024 * 1024),
            name="moe_exchange",
        )(expert_ids.reshape(1, rows), slot_ids.reshape(1, rows), tokens, w_gate, w_up, w_down)
        return (gate_weights * picked.astype(jnp.float32)).astype(bf16)

    return jax.shard_map(local_layer, mesh=mesh, in_specs=(tok_spec, tok_spec, tok_spec, tok_spec, weight_spec, weight_spec, weight_spec), out_specs=tok_spec, check_vma=False)
```

```python
import functools

import jax
import jax.numpy as jnp
from jax import lax
from jax.experimental import pallas as pl
from jax.experimental.pallas import tpu as pltpu
from jax.sharding import PartitionSpec as P

MESH = pl.DeviceIdType.MESH
CAP_FACTOR = 2
CORES = 2
LANES = 128
GROUP_ROWS = 256
PICK_MSGS = 2
VMEM_MIB = 52
X, Y = 0, 1


def capacity(rows, top_k, experts):
    return ((CAP_FACTOR * rows * top_k + 8 * experts - 1) // (8 * experts)) * 8


def far_first(n):
    return sorted(range(1, n), key=lambda d: -min(d, n - d))


class Plan:
    def __init__(self, nodes, chips, cap):
        self.size = {X: chips, Y: nodes}
        self.cap, self.half = cap, cap // 2
        self.msgs = [(a, d, c) for c in range(CORES) for i in range(max(nodes, chips) - 1) for a in (X, Y)
                     for d in far_first(self.size[a])[i:i + 1]]
        self.pieces = [(m, q) for m, (a, d, c) in enumerate(self.msgs) for q in far_first(self.size[1 - a])]
        self.piece_base = (2 + len(self.msgs)) * cap
        self.rows = self.piece_base + len(self.pieces) * self.half

    def direct_rows(self, m):
        return pl.ds((2 + m) * self.cap, self.cap)

    def piece_rows(self, k):
        return pl.ds(self.piece_base + k * self.half, self.half)

    def pieces_of(self, m):
        return [k for k, (mm, _) in enumerate(self.pieces) if mm == m]

    def spans(self):
        out = [(0, self.cap, (0, 0, 0), 0), (self.cap, self.cap, (0, 0, 1), 0)]
        for m, (a, d, c) in enumerate(self.msgs):
            out.append(((2 + m) * self.cap, self.cap, (0, d, c) if a == X else (d, 0, c), 0))
        for k, (m, q) in enumerate(self.pieces):
            a, d, c = self.msgs[m]
            out.append((self.piece_base + k * self.half, self.half, (q, d, c) if a == X else (d, q, c), 0 if a == X else self.half))
        return out


def kernel(plan, ids_hbm, slots_hbm, gates_hbm, tok_hbm, wg_hbm, wu_hbm, wd_hbm, acc, hot_ref, last_ref, gate_b,
           ids_ref, slots_ref, gates_ref, tok, wg, wu, wd, send, stage, recv, hid, y, stage2, ret, pos_b,
           in_sem, w_sem, s_rel, r_rel, s_dir, r_dir, s_fwd, r_fwd, s_rdir, r_rdir, s_rpc, r_rpc, s_rfw, r_rfw):
    rows = tok.shape[0]
    cap, half = plan.cap, plan.half
    nodes, chips = plan.size[Y], plan.size[X]
    data, node, exp = lax.axis_index("data"), lax.axis_index("node"), lax.axis_index("expert")
    chip, core = exp // CORES, lax.rem(exp, CORES)
    n_msgs, n_pieces = len(plan.msgs), len(plan.pieces)

    def place(dn, dx, flip):
        n, x = lax.rem(node + dn % nodes, nodes), lax.rem(chip + dx % chips, chips)
        return n, x * CORES + lax.rem(core + flip, CORES)

    def hop(axis, d, flip):
        n, e = place(0, d, flip) if axis == X else place(d, 0, flip)
        return (data, n, e)

    def first_slot(offset, slot):
        n, e = place(*offset)
        return (n * (chips * CORES) + e) * cap + slot

    def remote(src, dst, s, r, to):
        return pltpu.make_async_remote_copy(src, dst, s, r, device_id=to, device_id_type=MESH)

    def relay(m):
        ks = plan.pieces_of(m)
        part = pl.ds(ks[0] * half, len(ks) * half)
        a, d, c = plan.msgs[m]
        return remote(send.at[pl.ds(plan.piece_base + ks[0] * half, len(ks) * half)], stage.at[part], s_rel.at[m], r_rel.at[m], hop(a, d, c))

    def forward(k):
        m, q = plan.pieces[k]
        return remote(stage.at[pl.ds(k * half, half)], recv.at[plan.piece_rows(k)], s_fwd.at[k], r_fwd.at[k], hop(1 - plan.msgs[m][0], q, 0))

    def direct(m, src, dst, s, r, sign):
        if m < 0:
            part, to = pl.ds(cap, cap), hop(X, 0, 1)
        else:
            a, d, c = plan.msgs[m]
            part, to = plan.direct_rows(m), hop(a, sign * d, c)
        return remote(src.at[part], dst.at[part], s.at[m + 1], r.at[m + 1], to)

    def out_direct(m):
        return direct(m, send, recv, s_dir, r_dir, 1)

    def back_direct(m):
        return direct(m, y, ret, s_rdir, r_rdir, -1)

    def back_piece(k):
        a, d, c = plan.msgs[plan.pieces[k][0]]
        return remote(y.at[plan.piece_rows(k)], stage2.at[pl.ds(k * half, half)], s_rpc.at[k], r_rpc.at[k], hop(a, -d, c))

    def back_forward(k):
        m, q = plan.pieces[k]
        return remote(stage2.at[pl.ds(k * half, half)], ret.at[plan.piece_rows(k)], s_rfw.at[k], r_rfw.at[k], hop(1 - plan.msgs[m][0], -q, 0))

    barrier = pltpu.get_barrier_semaphore()
    near = [(X, 0, 1)] + plan.msgs
    for a, d, c in near:
        pl.semaphore_signal(barrier, inc=1, device_id=hop(a, d, c), device_id_type=MESH)
    in_copies = [pltpu.make_async_copy(h, v, in_sem.at[i])
                 for i, (h, v) in enumerate(((ids_hbm, ids_ref), (slots_hbm, slots_ref), (tok_hbm, tok), (gates_hbm, gates_ref)))]
    for c in in_copies:
        c.start()
    w_copies = [pltpu.make_async_copy(h.at[0], v, w_sem.at[i]) for i, (h, v) in enumerate(((wg_hbm, wg), (wu_hbm, wu), (wd_hbm, wd)))]

    for c in in_copies:
        c.wait()
    for c in w_copies:
        c.start()
    ids, slots = ids_ref[...], slots_ref[...]
    pos = jnp.where(slots >= 0, ids * cap + slots, -1)
    spans = plan.spans()

    def pick(lo, hi):
        parts = [s for s in spans if lo <= s[0] < hi]
        hot = [jnp.where(pos - first_slot(off, slot) == lax.broadcasted_iota(jnp.int32, (size, rows), 0), 1.0, 0.0).astype(jnp.bfloat16)
               for _, size, off, slot in parts]
        got = jnp.dot(jnp.concatenate(hot, axis=0), tok[...], preferred_element_type=jnp.float32).astype(jnp.bfloat16)
        if lo == 0:
            recv[pl.ds(0, cap)] = got[:cap]
        send[pl.ds(lo, hi - lo)] = got

    todo = []
    for m in range(0, n_msgs, PICK_MSGS):
        ms = list(range(m, min(m + PICK_MSGS, n_msgs)))
        ks = [k for mm in ms for k in plan.pieces_of(mm)]
        todo.append((plan.piece_base + ks[0] * half, plan.piece_base + (ks[-1] + 1) * half, [relay(mm) for mm in ms]))
    for lo in range(0, plan.piece_base, GROUP_ROWS):
        hi = min(lo + GROUP_ROWS, plan.piece_base)
        todo.append((lo, hi, [out_direct(m) for m in range(-1, n_msgs) if lo <= (2 + m) * cap < hi]))
    for i, (lo, hi, _) in enumerate(todo):
        pick(lo, hi)
        if i == 1:
            pl.semaphore_wait(barrier, len(near))
        if i >= 1:
            for c in todo[i - 1][2]:
                c.start()
    for c in todo[-1][2]:
        c.start()

    for b in range(rows // LANES):
        pos_b[pl.ds(b * LANES, LANES), :] = jnp.transpose(jnp.broadcast_to(pos[:, b * LANES:(b + 1) * LANES], (LANES, LANES)))
        gate_b[pl.ds(b * LANES, LANES), :] = jnp.transpose(jnp.broadcast_to(gates_ref[:, b * LANES:(b + 1) * LANES], (LANES, LANES)))

    for m in range(n_msgs):
        relay(m).wait_recv()
        for k in plan.pieces_of(m):
            forward(k).start()
    for c in w_copies:
        c.wait()

    n_groups = plan.rows // GROUP_ROWS

    def in_group(g):
        lo, hi = g * GROUP_ROWS, (g + 1) * GROUP_ROWS
        ms = [m for m in range(-1, n_msgs) if lo <= (2 + m) * cap < hi]
        ks = [k for k in range(n_pieces) if lo <= plan.piece_base + k * half < hi]
        return ms, ks

    def expert_group(g, carry):
        for j in range(n_groups):
            @pl.when(g == j)
            def _(j=j):
                ms, ks = in_group(j)
                for m in ms:
                    out_direct(m).wait_recv()
                for k in ks:
                    forward(k).wait_recv()
        at = pl.ds(pl.multiple_of(g * GROUP_ROWS, GROUP_ROWS), GROUP_ROWS)
        a = jnp.dot(recv[at], wg[...], preferred_element_type=jnp.float32)
        b = jnp.dot(recv[at], wu[...], preferred_element_type=jnp.float32)
        hid[...] = (jax.nn.silu(a) * b).astype(jnp.bfloat16)
        y[at] = jnp.dot(hid[...], wd[...], preferred_element_type=jnp.float32).astype(jnp.bfloat16)
        for j in range(n_groups):
            @pl.when(g == j)
            def _(j=j):
                ms, ks = in_group(j)
                for m in ms:
                    back_direct(m).start()
                for k in ks:
                    back_piece(k).start()
        return carry

    lax.fori_loop(0, n_groups, expert_group, 0)
    ret[pl.ds(0, cap)] = y[pl.ds(0, cap)]

    lane = lax.broadcasted_iota(jnp.int32, (1, LANES), 1)

    def hot_rows(lo, hi):
        hots = []
        for at in range(lo, hi, LANES):
            want = None
            for first, size, off, slot in spans:
                if at <= first < at + LANES:
                    here = lane - (first - at) + first_slot(off, slot)
                    want = here if want is None else jnp.where(lane >= first - at, here, want)
            hots.append(jnp.where(pos_b[...] == want, 1.0, 0.0).astype(jnp.bfloat16))
        return jnp.concatenate(hots, axis=1) if len(hots) > 1 else hots[0]

    def picked(lo, hi):
        return jnp.dot(hot_rows(lo, hi), ret[pl.ds(lo, hi - lo)], preferred_element_type=jnp.float32)

    split = n_pieces // 3
    for k in range(split):
        back_piece(k).wait_recv()
        back_forward(k).start()
    for m in range(-1, n_msgs):
        back_direct(m).wait_recv()
    acc[...] = picked(0, plan.piece_base)
    for k in range(split, n_pieces):
        back_piece(k).wait_recv()
        back_forward(k).start()
    last = plan.rows - LANES
    hot_ref[...] = hot_rows(last, plan.rows)
    lo = plan.piece_base
    for hi in (lo + n_pieces // 2 // 4 * 4 * half, last):
        for k in range(n_pieces):
            if lo <= plan.piece_base + k * half < hi:
                back_forward(k).wait_recv()
        acc[...] += picked(lo, hi)
        lo = hi
    for k in range(n_pieces):
        if plan.piece_base + k * half >= last:
            back_forward(k).wait_recv()
    last_ref[...] = ret[pl.ds(last, LANES)]

    for m in range(n_msgs):
        relay(m).wait_send()
    for m in range(-1, n_msgs):
        out_direct(m).wait_send()
        back_direct(m).wait_send()
    for k in range(n_pieces):
        forward(k).wait_send()
        back_piece(k).wait_send()
        back_forward(k).wait_send()


def finish(acc, hot, last, gate, out_hbm, buf, sem):
    rows, width = acc.shape
    step = rows // 4
    copies = []
    for i in range(4):
        at = pl.ds(i * step, step)
        total = acc[at] + jnp.dot(hot[at], last[...], preferred_element_type=jnp.float32)
        for j in range(width // LANES):
            buf[at, j * LANES:(j + 1) * LANES] = (gate[at] * total[:, j * LANES:(j + 1) * LANES]).astype(buf.dtype)
        copies.append(pltpu.make_async_copy(buf.at[at], out_hbm.at[at], sem.at[i]))
        copies[-1].start()
    for c in copies:
        c.wait()


def solution(mesh):
    nodes, chips = mesh.shape["node"], mesh.shape["expert"] // CORES
    tok_spec = P(("data", "node", "expert"), None)
    weight_spec = P(("node", "expert"), None, None)

    def local_layer(tokens, expert_ids, gate_weights, slot_ids, w_gate, w_up, w_down):
        rows, width = tokens.shape
        ff = w_gate.shape[2]
        cap = capacity(rows, expert_ids.shape[1], nodes * chips * CORES * w_gate.shape[0])
        plan = Plan(nodes, chips, cap)
        n_msgs, n_pieces = len(plan.msgs), len(plan.pieces)
        vmem, hbm = pl.BlockSpec(memory_space=pltpu.VMEM), pl.BlockSpec(memory_space=pl.ANY)
        bf16 = jnp.bfloat16
        sem = lambda n: pltpu.SemaphoreType.DMA((n,))
        parts = pl.pallas_call(
            functools.partial(kernel, plan),
            out_shape=[pltpu.VMEM((rows, width), jnp.float32), pltpu.VMEM((rows, LANES), bf16), pltpu.VMEM((LANES, width), bf16),
                       pltpu.VMEM((rows, LANES), jnp.float32)],
            in_specs=[hbm] * 7,
            out_specs=[vmem] * 4,
            scratch_shapes=[
                pltpu.VMEM((1, rows), jnp.int32),
                pltpu.VMEM((1, rows), jnp.int32),
                pltpu.VMEM((1, rows), jnp.float32),
                pltpu.VMEM((rows, width), bf16),
                pltpu.VMEM((width, ff), bf16),
                pltpu.VMEM((width, ff), bf16),
                pltpu.VMEM((ff, width), bf16),
                pltpu.VMEM((plan.rows, width), bf16),
                pltpu.VMEM((n_pieces * plan.half, width), bf16),
                pltpu.VMEM((plan.rows, width), bf16),
                pltpu.VMEM((GROUP_ROWS, ff), bf16),
                pltpu.VMEM((plan.rows, width), bf16),
                pltpu.VMEM((n_pieces * plan.half, width), bf16),
                pltpu.VMEM((plan.rows, width), bf16),
                pltpu.VMEM((rows, LANES), jnp.int32),
                sem(4), sem(3), sem(n_msgs), sem(n_msgs), sem(n_msgs + 1), sem(n_msgs + 1), sem(n_pieces), sem(n_pieces),
                sem(n_msgs + 1), sem(n_msgs + 1), sem(n_pieces), sem(n_pieces), sem(n_pieces), sem(n_pieces),
            ],
            compiler_params=pltpu.CompilerParams(collective_id=0, has_side_effects=True, vmem_limit_bytes=VMEM_MIB * 1024 * 1024),
            name="moe_exchange",
        )(expert_ids.reshape(1, rows), slot_ids.reshape(1, rows), gate_weights.reshape(1, rows), tokens, w_gate, w_up, w_down)
        return pl.pallas_call(
            finish,
            out_shape=jax.ShapeDtypeStruct((rows, width), bf16),
            in_specs=[vmem] * 4,
            out_specs=hbm,
            scratch_shapes=[pltpu.VMEM((rows, width), bf16), sem(4)],
            compiler_params=pltpu.CompilerParams(vmem_limit_bytes=8 * 1024 * 1024),
            name="moe_finish",
        )(*parts)

    return jax.shard_map(local_layer, mesh=mesh, in_specs=(tok_spec, tok_spec, tok_spec, tok_spec, weight_spec, weight_spec, weight_spec), out_specs=tok_spec, check_vma=False)
```

```python
import functools

import jax
import jax.numpy as jnp
from jax import lax
from jax.experimental import pallas as pl
from jax.experimental.pallas import tpu as pltpu
from jax.sharding import PartitionSpec as P

MESH = pl.DeviceIdType.MESH
CAP_FACTOR = 2
CORES = 2
LANES = 128
GROUP_ROWS = 256
PICK_MSGS = 2
VMEM_MIB = 52
X, Y = 0, 1


def capacity(rows, top_k, experts):
    return ((CAP_FACTOR * rows * top_k + 8 * experts - 1) // (8 * experts)) * 8


def far_first(n):
    return sorted(range(1, n), key=lambda d: -min(d, n - d))


class Plan:
    def __init__(self, nodes, chips, cap):
        self.size = {X: chips, Y: nodes}
        self.cap, self.half = cap, cap // 2
        self.msgs = [(a, d, c) for c in range(CORES) for i in range(max(nodes, chips) - 1) for a in (X, Y)
                     for d in far_first(self.size[a])[i:i + 1]]
        self.pieces = [(m, q) for m, (a, d, c) in enumerate(self.msgs) for q in far_first(self.size[1 - a])]
        self.piece_base = (2 + len(self.msgs)) * cap
        self.rows = self.piece_base + len(self.pieces) * self.half

    def direct_rows(self, m):
        return pl.ds((2 + m) * self.cap, self.cap)

    def piece_rows(self, k):
        return pl.ds(self.piece_base + k * self.half, self.half)

    def pieces_of(self, m):
        return [k for k, (mm, _) in enumerate(self.pieces) if mm == m]

    def spans(self):
        out = [(0, self.cap, (0, 0, 0), 0), (self.cap, self.cap, (0, 0, 1), 0)]
        for m, (a, d, c) in enumerate(self.msgs):
            out.append(((2 + m) * self.cap, self.cap, (0, d, c) if a == X else (d, 0, c), 0))
        for k, (m, q) in enumerate(self.pieces):
            a, d, c = self.msgs[m]
            out.append((self.piece_base + k * self.half, self.half, (q, d, c) if a == X else (d, q, c), 0 if a == X else self.half))
        return out


def kernel(plan, ids_hbm, slots_hbm, gates_hbm, tok_hbm, wg_hbm, wu_hbm, wd_hbm, acc, hot_ref, last_ref, gate_b,
           ids_ref, slots_ref, gates_ref, tok, wg, wu, wd, send, stage, recv, hid, y, stage2, ret, pos_b,
           in_sem, w_sem, sent, r_rel, r_grp, r_rdir, r_rpc, r_ret):
    rows = tok.shape[0]
    cap, half = plan.cap, plan.half
    nodes, chips = plan.size[Y], plan.size[X]
    data, node, exp = lax.axis_index("data"), lax.axis_index("node"), lax.axis_index("expert")
    chip, core = exp // CORES, lax.rem(exp, CORES)
    n_msgs, n_pieces = len(plan.msgs), len(plan.pieces)

    def place(dn, dx, flip):
        n, x = lax.rem(node + dn % nodes, nodes), lax.rem(chip + dx % chips, chips)
        return n, x * CORES + lax.rem(core + flip, CORES)

    def hop(axis, d, flip):
        n, e = place(0, d, flip) if axis == X else place(d, 0, flip)
        return (data, n, e)

    def first_slot(offset, slot):
        n, e = place(*offset)
        return (n * (chips * CORES) + e) * cap + slot

    def remote(src, dst, s, r, to):
        return pltpu.make_async_remote_copy(src, dst, s, r, device_id=to, device_id_type=MESH)

    def relay(m):
        ks = plan.pieces_of(m)
        part = pl.ds(ks[0] * half, len(ks) * half)
        a, d, c = plan.msgs[m]
        return remote(send.at[pl.ds(plan.piece_base + ks[0] * half, len(ks) * half)], stage.at[part], sent.at[0], r_rel.at[m], hop(a, d, c))

    def forward(k):
        m, q = plan.pieces[k]
        return remote(stage.at[pl.ds(k * half, half)], recv.at[plan.piece_rows(k)], sent.at[1], r_grp.at[group_of(plan.piece_base + k * half)], hop(1 - plan.msgs[m][0], q, 0))

    last = plan.rows - LANES
    cut = plan.piece_base + (n_pieces // 2 // 4 * 4) * half

    def ret_part(row):
        return 0 if row < cut else 1 if row < last else 2

    def arrived(ref, lo, hi, sem):
        part = ref.at[pl.ds(lo, hi - lo)]
        pltpu.make_async_copy(part, part, sem).wait()

    def group_of(row):
        return row // GROUP_ROWS

    def direct(m, src, dst, s, r, sign):
        if m < 0:
            part, to = pl.ds(cap, cap), hop(X, 0, 1)
        else:
            a, d, c = plan.msgs[m]
            part, to = plan.direct_rows(m), hop(a, sign * d, c)
        return remote(src.at[part], dst.at[part], s, r, to)

    def out_direct(m):
        return direct(m, send, recv, sent.at[2], r_grp.at[group_of((2 + m) * cap)], 1)

    def back_direct(m):
        return direct(m, y, ret, sent.at[3], r_rdir, -1)

    def back_piece(k):
        a, d, c = plan.msgs[plan.pieces[k][0]]
        return remote(y.at[plan.piece_rows(k)], stage2.at[pl.ds(k * half, half)], sent.at[4], r_rpc.at[plan.pieces[k][0]], hop(a, -d, c))

    def back_forward(k):
        m, q = plan.pieces[k]
        return remote(stage2.at[pl.ds(k * half, half)], ret.at[plan.piece_rows(k)], sent.at[5], r_ret.at[ret_part(plan.piece_base + k * half)], hop(1 - plan.msgs[m][0], -q, 0))

    barrier = pltpu.get_barrier_semaphore()
    near = [(X, 0, 1)] + plan.msgs
    for a, d, c in near:
        pl.semaphore_signal(barrier, inc=1, device_id=hop(a, d, c), device_id_type=MESH)
    in_copies = [pltpu.make_async_copy(h, v, in_sem.at[i])
                 for i, (h, v) in enumerate(((ids_hbm, ids_ref), (slots_hbm, slots_ref), (tok_hbm, tok), (gates_hbm, gates_ref)))]
    for c in in_copies:
        c.start()
    w_copies = [pltpu.make_async_copy(h.at[0], v, w_sem.at[i]) for i, (h, v) in enumerate(((wg_hbm, wg), (wu_hbm, wu), (wd_hbm, wd)))]

    for c in in_copies:
        c.wait()
    for c in w_copies:
        c.start()
    ids, slots = ids_ref[...], slots_ref[...]
    pos = jnp.where(slots >= 0, ids * cap + slots, -1)
    spans = plan.spans()

    def pick(lo, hi):
        parts = [s for s in spans if lo <= s[0] < hi]
        hot = [jnp.where(pos - first_slot(off, slot) == lax.broadcasted_iota(jnp.int32, (size, rows), 0), 1.0, 0.0).astype(jnp.bfloat16)
               for _, size, off, slot in parts]
        got = jnp.dot(jnp.concatenate(hot, axis=0), tok[...], preferred_element_type=jnp.float32).astype(jnp.bfloat16)
        if lo == 0:
            recv[pl.ds(0, cap)] = got[:cap]
        send[pl.ds(lo, hi - lo)] = got

    todo = []
    for m in range(0, n_msgs, PICK_MSGS):
        ms = list(range(m, min(m + PICK_MSGS, n_msgs)))
        ks = [k for mm in ms for k in plan.pieces_of(mm)]
        todo.append((plan.piece_base + ks[0] * half, plan.piece_base + (ks[-1] + 1) * half, [relay(mm) for mm in ms]))
    for lo in range(0, plan.piece_base, GROUP_ROWS):
        hi = min(lo + GROUP_ROWS, plan.piece_base)
        todo.append((lo, hi, [out_direct(m) for m in range(-1, n_msgs) if lo <= (2 + m) * cap < hi]))
    for i, (lo, hi, _) in enumerate(todo):
        pick(lo, hi)
        if i == 1:
            pl.semaphore_wait(barrier, len(near))
        if i >= 1:
            for c in todo[i - 1][2]:
                c.start()
    for c in todo[-1][2]:
        c.start()

    for b in range(rows // LANES):
        pos_b[pl.ds(b * LANES, LANES), :] = jnp.transpose(jnp.broadcast_to(pos[:, b * LANES:(b + 1) * LANES], (LANES, LANES)))
        gate_b[pl.ds(b * LANES, LANES), :] = jnp.transpose(jnp.broadcast_to(gates_ref[:, b * LANES:(b + 1) * LANES], (LANES, LANES)))

    for m in range(n_msgs):
        relay(m).wait_recv()
        for k in plan.pieces_of(m):
            forward(k).start()
    for c in w_copies:
        c.wait()

    n_groups = plan.rows // GROUP_ROWS

    def in_group(g):
        lo, hi = g * GROUP_ROWS, (g + 1) * GROUP_ROWS
        ms = [m for m in range(-1, n_msgs) if lo <= (2 + m) * cap < hi]
        ks = [k for k in range(n_pieces) if lo <= plan.piece_base + k * half < hi]
        return ms, ks

    def expert_group(g, carry):
        for j in range(n_groups):
            @pl.when(g == j)
            def _(j=j):
                arrived(recv, max(j * GROUP_ROWS, cap), (j + 1) * GROUP_ROWS, r_grp.at[j])
        at = pl.ds(pl.multiple_of(g * GROUP_ROWS, GROUP_ROWS), GROUP_ROWS)
        a = jnp.dot(recv[at], wg[...], preferred_element_type=jnp.float32)
        b = jnp.dot(recv[at], wu[...], preferred_element_type=jnp.float32)
        hid[...] = (jax.nn.silu(a) * b).astype(jnp.bfloat16)
        y[at] = jnp.dot(hid[...], wd[...], preferred_element_type=jnp.float32).astype(jnp.bfloat16)
        for j in range(n_groups):
            @pl.when(g == j)
            def _(j=j):
                ms, ks = in_group(j)
                for m in ms:
                    back_direct(m).start()
                for k in ks:
                    back_piece(k).start()
        return carry

    lax.fori_loop(0, n_groups, expert_group, 0)
    ret[pl.ds(0, cap)] = y[pl.ds(0, cap)]

    lane = lax.broadcasted_iota(jnp.int32, (1, LANES), 1)

    def hot_rows(lo, hi):
        hots = []
        for at in range(lo, hi, LANES):
            want = None
            for first, size, off, slot in spans:
                if at <= first < at + LANES:
                    here = lane - (first - at) + first_slot(off, slot)
                    want = here if want is None else jnp.where(lane >= first - at, here, want)
            hots.append(jnp.where(pos_b[...] == want, 1.0, 0.0).astype(jnp.bfloat16))
        return jnp.concatenate(hots, axis=1) if len(hots) > 1 else hots[0]

    def picked(lo, hi):
        return jnp.dot(hot_rows(lo, hi), ret[pl.ds(lo, hi - lo)], preferred_element_type=jnp.float32)

    def send_back(ms):
        for m in ms:
            ks = plan.pieces_of(m)
            arrived(stage2, ks[0] * half, (ks[-1] + 1) * half, r_rpc.at[m])
            for k in ks:
                back_forward(k).start()

    send_back(range(n_msgs // 3))
    arrived(ret, cap, plan.piece_base, r_rdir)
    acc[...] = picked(0, plan.piece_base)
    send_back(range(n_msgs // 3, n_msgs))
    hot_ref[...] = hot_rows(last, plan.rows)
    for lo, hi in ((plan.piece_base, cut), (cut, last)):
        arrived(ret, lo, hi, r_ret.at[ret_part(lo)])
        acc[...] += picked(lo, hi)
    arrived(ret, last, plan.rows, r_ret.at[2])
    last_ref[...] = ret[pl.ds(last, LANES)]

    n_rows = plan.rows - plan.piece_base
    for i, (lo, hi) in enumerate(((0, n_rows), (0, n_rows), (cap, plan.piece_base), (cap, plan.piece_base), (0, n_rows), (0, n_rows))):
        arrived(send, lo, hi, sent.at[i])


def finish(acc, hot, last, gate, out_hbm, buf, sem):
    rows, width = acc.shape
    step = rows // 4
    copies = []
    for i in range(4):
        at = pl.ds(i * step, step)
        total = acc[at] + jnp.dot(hot[at], last[...], preferred_element_type=jnp.float32)
        for j in range(width // LANES):
            buf[at, j * LANES:(j + 1) * LANES] = (gate[at] * total[:, j * LANES:(j + 1) * LANES]).astype(buf.dtype)
        copies.append(pltpu.make_async_copy(buf.at[at], out_hbm.at[at], sem.at[i]))
        copies[-1].start()
    for c in copies:
        c.wait()


def solution(mesh):
    nodes, chips = mesh.shape["node"], mesh.shape["expert"] // CORES
    tok_spec = P(("data", "node", "expert"), None)
    weight_spec = P(("node", "expert"), None, None)

    def local_layer(tokens, expert_ids, gate_weights, slot_ids, w_gate, w_up, w_down):
        rows, width = tokens.shape
        ff = w_gate.shape[2]
        cap = capacity(rows, expert_ids.shape[1], nodes * chips * CORES * w_gate.shape[0])
        plan = Plan(nodes, chips, cap)
        n_msgs, n_pieces = len(plan.msgs), len(plan.pieces)
        vmem, hbm = pl.BlockSpec(memory_space=pltpu.VMEM), pl.BlockSpec(memory_space=pl.ANY)
        bf16 = jnp.bfloat16
        sem = lambda n: pltpu.SemaphoreType.DMA((n,))
        parts = pl.pallas_call(
            functools.partial(kernel, plan),
            out_shape=[pltpu.VMEM((rows, width), jnp.float32), pltpu.VMEM((rows, LANES), bf16), pltpu.VMEM((LANES, width), bf16),
                       pltpu.VMEM((rows, LANES), jnp.float32)],
            in_specs=[hbm] * 7,
            out_specs=[vmem] * 4,
            scratch_shapes=[
                pltpu.VMEM((1, rows), jnp.int32),
                pltpu.VMEM((1, rows), jnp.int32),
                pltpu.VMEM((1, rows), jnp.float32),
                pltpu.VMEM((rows, width), bf16),
                pltpu.VMEM((width, ff), bf16),
                pltpu.VMEM((width, ff), bf16),
                pltpu.VMEM((ff, width), bf16),
                pltpu.VMEM((plan.rows, width), bf16),
                pltpu.VMEM((n_pieces * plan.half, width), bf16),
                pltpu.VMEM((plan.rows, width), bf16),
                pltpu.VMEM((GROUP_ROWS, ff), bf16),
                pltpu.VMEM((plan.rows, width), bf16),
                pltpu.VMEM((n_pieces * plan.half, width), bf16),
                pltpu.VMEM((plan.rows, width), bf16),
                pltpu.VMEM((rows, LANES), jnp.int32),
                sem(4), sem(3), sem(6), sem(n_msgs), sem(plan.rows // GROUP_ROWS), pltpu.SemaphoreType.DMA, sem(n_msgs), sem(3),
            ],
            compiler_params=pltpu.CompilerParams(collective_id=0, has_side_effects=True, vmem_limit_bytes=VMEM_MIB * 1024 * 1024),
            name="moe_exchange",
        )(expert_ids.reshape(1, rows), slot_ids.reshape(1, rows), gate_weights.reshape(1, rows), tokens, w_gate, w_up, w_down)
        return pl.pallas_call(
            finish,
            out_shape=jax.ShapeDtypeStruct((rows, width), bf16),
            in_specs=[vmem] * 4,
            out_specs=hbm,
            scratch_shapes=[pltpu.VMEM((rows, width), bf16), sem(4)],
            compiler_params=pltpu.CompilerParams(vmem_limit_bytes=8 * 1024 * 1024),
            name="moe_finish",
        )(*parts)

    return jax.shard_map(local_layer, mesh=mesh, in_specs=(tok_spec, tok_spec, tok_spec, tok_spec, weight_spec, weight_spec, weight_spec), out_specs=tok_spec, check_vma=False)
```

```python
import functools

import jax
import jax.numpy as jnp
from jax import lax
from jax.experimental import pallas as pl
from jax.experimental.pallas import tpu as pltpu
from jax.sharding import PartitionSpec as P

MESH = pl.DeviceIdType.MESH
CAP_FACTOR = 2
CORES = 2
LANES = 128
GROUP_ROWS = 256
PICK_MSGS = 2
VMEM_MIB = 52
OUT_CHUNKS = 8
X, Y = 0, 1


def capacity(rows, top_k, experts):
    return ((CAP_FACTOR * rows * top_k + 8 * experts - 1) // (8 * experts)) * 8


def far_first(n):
    return sorted(range(1, n), key=lambda d: -min(d, n - d))


class Plan:
    def __init__(self, nodes, chips, cap):
        self.size = {X: chips, Y: nodes}
        self.cap, self.half = cap, cap // 2
        self.msgs = [(a, d, c) for c in range(CORES) for i in range(max(nodes, chips) - 1) for a in (X, Y)
                     for d in far_first(self.size[a])[i:i + 1]]
        self.pieces = [(m, q) for m, (a, d, c) in enumerate(self.msgs) for q in far_first(self.size[1 - a])]
        self.piece_base = (2 + len(self.msgs)) * cap
        self.rows = self.piece_base + len(self.pieces) * self.half

    def direct_rows(self, m):
        return pl.ds((2 + m) * self.cap, self.cap)

    def piece_rows(self, k):
        return pl.ds(self.piece_base + k * self.half, self.half)

    def pieces_of(self, m):
        return [k for k, (mm, _) in enumerate(self.pieces) if mm == m]

    def spans(self):
        out = [(0, self.cap, (0, 0, 0), 0), (self.cap, self.cap, (0, 0, 1), 0)]
        for m, (a, d, c) in enumerate(self.msgs):
            out.append(((2 + m) * self.cap, self.cap, (0, d, c) if a == X else (d, 0, c), 0))
        for k, (m, q) in enumerate(self.pieces):
            a, d, c = self.msgs[m]
            out.append((self.piece_base + k * self.half, self.half, (q, d, c) if a == X else (d, q, c), 0 if a == X else self.half))
        return out


def kernel(plan, ids_hbm, slots_hbm, gates_hbm, tok_hbm, wg_hbm, wu_hbm, wd_hbm, acc, hot_ref, last_ref, gate_b,
           ids_ref, slots_ref, gates_ref, tok, wg, wu, wd, send, stage, recv, hid, y, stage2, ret, pos_b,
           in_sem, w_sem, sent, r_rel, r_grp, r_rdir, r_rpc, r_ret):
    rows = tok.shape[0]
    cap, half = plan.cap, plan.half
    nodes, chips = plan.size[Y], plan.size[X]
    data, node, exp = lax.axis_index("data"), lax.axis_index("node"), lax.axis_index("expert")
    chip, core = exp // CORES, lax.rem(exp, CORES)
    n_msgs, n_pieces = len(plan.msgs), len(plan.pieces)

    def place(dn, dx, flip):
        n, x = lax.rem(node + dn % nodes, nodes), lax.rem(chip + dx % chips, chips)
        return n, x * CORES + lax.rem(core + flip, CORES)

    def hop(axis, d, flip):
        n, e = place(0, d, flip) if axis == X else place(d, 0, flip)
        return (data, n, e)

    def first_slot(offset, slot):
        n, e = place(*offset)
        return (n * (chips * CORES) + e) * cap + slot

    def remote(src, dst, s, r, to):
        return pltpu.make_async_remote_copy(src, dst, s, r, device_id=to, device_id_type=MESH)

    def relay(m):
        ks = plan.pieces_of(m)
        part = pl.ds(ks[0] * half, len(ks) * half)
        a, d, c = plan.msgs[m]
        return remote(send.at[pl.ds(plan.piece_base + ks[0] * half, len(ks) * half)], stage.at[part], sent.at[0], r_rel.at[m // 2], hop(a, d, c))

    def forward(k):
        m, q = plan.pieces[k]
        return remote(stage.at[pl.ds(k * half, half)], recv.at[plan.piece_rows(k)], sent.at[1], r_grp.at[group_of(plan.piece_base + k * half)], hop(1 - plan.msgs[m][0], q, 0))

    last = plan.rows - LANES
    cut = plan.piece_base + (n_pieces // 2 // 4 * 4) * half

    batches = [range(0, n_msgs // 2), range(n_msgs // 2, n_msgs - 3)] + [range(m, m + 1) for m in range(n_msgs - 3, n_msgs)]

    def batch_of(m):
        return next(i for i, b in enumerate(batches) if m in b)

    def ret_part(row):
        return 0 if row < cut else 1 if row < last else 2

    def arrived(ref, lo, hi, sem):
        part = ref.at[pl.ds(lo, hi - lo)]
        pltpu.make_async_copy(part, part, sem).wait()

    def group_of(row):
        return row // GROUP_ROWS

    def direct(m, src, dst, s, r, sign):
        if m < 0:
            part, to = pl.ds(cap, cap), hop(X, 0, 1)
        else:
            a, d, c = plan.msgs[m]
            part, to = plan.direct_rows(m), hop(a, sign * d, c)
        return remote(src.at[part], dst.at[part], s, r, to)

    def out_direct(m):
        return direct(m, send, recv, sent.at[2], r_grp.at[group_of((2 + m) * cap)], 1)

    def back_direct(m):
        return direct(m, y, ret, sent.at[3], r_rdir, -1)

    def back_piece(k):
        a, d, c = plan.msgs[plan.pieces[k][0]]
        return remote(y.at[plan.piece_rows(k)], stage2.at[pl.ds(k * half, half)], sent.at[4], r_rpc.at[batch_of(plan.pieces[k][0])], hop(a, -d, c))

    def back_forward(k):
        m, q = plan.pieces[k]
        return remote(stage2.at[pl.ds(k * half, half)], ret.at[plan.piece_rows(k)], sent.at[5], r_ret.at[ret_part(plan.piece_base + k * half)], hop(1 - plan.msgs[m][0], -q, 0))

    barrier = pltpu.get_barrier_semaphore()
    near = [(X, 0, 1)] + plan.msgs
    for a, d, c in near:
        pl.semaphore_signal(barrier, inc=1, device_id=hop(a, d, c), device_id_type=MESH)
    in_copies = [pltpu.make_async_copy(h, v, in_sem.at[i])
                 for i, (h, v) in enumerate(((ids_hbm, ids_ref), (slots_hbm, slots_ref), (tok_hbm, tok), (gates_hbm, gates_ref)))]
    for c in in_copies:
        c.start()
    w_copies = [pltpu.make_async_copy(h.at[0], v, w_sem.at[i]) for i, (h, v) in enumerate(((wg_hbm, wg), (wu_hbm, wu), (wd_hbm, wd)))]

    for c in in_copies:
        c.wait()
    for c in w_copies:
        c.start()
    ids, slots = ids_ref[...], slots_ref[...]
    pos = jnp.where(slots >= 0, ids * cap + slots, -1)
    spans = plan.spans()

    def pick(lo, hi):
        parts = [s for s in spans if lo <= s[0] < hi]
        hot = [jnp.where(pos - first_slot(off, slot) == lax.broadcasted_iota(jnp.int32, (size, rows), 0), 1.0, 0.0).astype(jnp.bfloat16)
               for _, size, off, slot in parts]
        got = jnp.dot(jnp.concatenate(hot, axis=0), tok[...], preferred_element_type=jnp.float32).astype(jnp.bfloat16)
        if lo == 0:
            recv[pl.ds(0, cap)] = got[:cap]
        send[pl.ds(lo, hi - lo)] = got

    todo = []
    for m in range(0, n_msgs, PICK_MSGS):
        ms = list(range(m, min(m + PICK_MSGS, n_msgs)))
        ks = [k for mm in ms for k in plan.pieces_of(mm)]
        todo.append((plan.piece_base + ks[0] * half, plan.piece_base + (ks[-1] + 1) * half, [relay(mm) for mm in ms]))
    for lo in range(0, plan.piece_base, GROUP_ROWS):
        hi = min(lo + GROUP_ROWS, plan.piece_base)
        todo.append((lo, hi, [out_direct(m) for m in range(-1, n_msgs) if lo <= (2 + m) * cap < hi]))
    for i, (lo, hi, _) in enumerate(todo):
        pick(lo, hi)
        if i == 1:
            pl.semaphore_wait(barrier, len(near))
        if i >= 1:
            for c in todo[i - 1][2]:
                c.start()
    for c in todo[-1][2]:
        c.start()

    for b in range(rows // LANES):
        pos_b[pl.ds(b * LANES, LANES), :] = jnp.transpose(jnp.broadcast_to(pos[:, b * LANES:(b + 1) * LANES], (LANES, LANES)))
        gate_b[pl.ds(b * LANES, LANES), :] = jnp.transpose(jnp.broadcast_to(gates_ref[:, b * LANES:(b + 1) * LANES], (LANES, LANES)))

    for i in range(n_msgs // 2):
        ks = plan.pieces_of(2 * i) + plan.pieces_of(2 * i + 1)
        arrived(stage, ks[0] * half, (ks[-1] + 1) * half, r_rel.at[i])
        for k in ks:
            forward(k).start()
    for c in w_copies:
        c.wait()

    n_groups = plan.rows // GROUP_ROWS

    def in_group(g):
        lo, hi = g * GROUP_ROWS, (g + 1) * GROUP_ROWS
        ms = [m for m in range(-1, n_msgs) if lo <= (2 + m) * cap < hi]
        ks = [k for k in range(n_pieces) if lo <= plan.piece_base + k * half < hi]
        return ms, ks

    def expert_group(g, carry):
        for j in range(n_groups):
            @pl.when(g == j)
            def _(j=j):
                arrived(recv, max(j * GROUP_ROWS, cap), (j + 1) * GROUP_ROWS, r_grp.at[j])
        at = pl.ds(pl.multiple_of(g * GROUP_ROWS, GROUP_ROWS), GROUP_ROWS)
        a = jnp.dot(recv[at], wg[...], preferred_element_type=jnp.float32)
        b = jnp.dot(recv[at], wu[...], preferred_element_type=jnp.float32)
        hid[...] = (jax.nn.silu(a) * b).astype(jnp.bfloat16)
        rounded = jnp.dot(hid[...], wd[...], preferred_element_type=jnp.float32).astype(jnp.bfloat16).astype(jnp.float32)
        y[at] = jnp.where(jnp.abs(rounded) < jnp.inf, rounded, 0.0).astype(jnp.bfloat16)
        for j in range(n_groups):
            @pl.when(g == j)
            def _(j=j):
                ms, ks = in_group(j)
                for m in ms:
                    back_direct(m).start()
                for k in ks:
                    back_piece(k).start()
        return carry

    lax.fori_loop(0, n_groups, expert_group, 0)
    ret[pl.ds(0, cap)] = y[pl.ds(0, cap)]

    lane = lax.broadcasted_iota(jnp.int32, (1, LANES), 1)

    def hot_rows(lo, hi):
        hots = []
        for at in range(lo, hi, LANES):
            want = None
            for first, size, off, slot in spans:
                if at <= first < at + LANES:
                    here = lane - (first - at) + first_slot(off, slot)
                    want = here if want is None else jnp.where(lane >= first - at, here, want)
            hots.append(jnp.where(pos_b[...] == want, 1.0, 0.0).astype(jnp.bfloat16))
        return jnp.concatenate(hots, axis=1) if len(hots) > 1 else hots[0]

    def picked(lo, hi):
        return jnp.dot(hot_rows(lo, hi), ret[pl.ds(lo, hi - lo)], preferred_element_type=jnp.float32)

    def send_back(ids):
        for i in ids:
            ks = [k for m in batches[i] for k in plan.pieces_of(m)]
            arrived(stage2, ks[0] * half, (ks[-1] + 1) * half, r_rpc.at[i])
            for k in ks:
                back_forward(k).start()

    send_back([0])
    arrived(ret, cap, plan.piece_base, r_rdir)
    acc[...] = picked(0, plan.piece_base)
    send_back(range(1, len(batches)))
    hot_ref[...] = hot_rows(last, plan.rows)
    for lo, hi in ((plan.piece_base, cut), (cut, last)):
        arrived(ret, lo, hi, r_ret.at[ret_part(lo)])
        acc[...] += picked(lo, hi)
    arrived(ret, last, plan.rows, r_ret.at[2])
    last_ref[...] = ret[pl.ds(last, LANES)]

    n_rows = plan.rows - plan.piece_base
    for i, (lo, hi) in enumerate(((0, n_rows), (0, n_rows), (cap, plan.piece_base), (cap, plan.piece_base), (0, n_rows), (0, n_rows))):
        arrived(send, lo, hi, sent.at[i])


def finish(acc, hot, last, gate, out_hbm, buf, sem):
    rows, width = acc.shape
    step = rows // OUT_CHUNKS
    for i in range(OUT_CHUNKS):
        at = pl.ds(i * step, step)
        total = acc[at] + jnp.dot(hot[at], last[...], preferred_element_type=jnp.float32)
        for j in range(width // LANES):
            buf[at, j * LANES:(j + 1) * LANES] = (gate[at] * total[:, j * LANES:(j + 1) * LANES]).astype(buf.dtype)
        pltpu.make_async_copy(buf.at[at], out_hbm.at[at], sem).start()
    pltpu.make_async_copy(buf, out_hbm, sem).wait()


def solution(mesh):
    nodes, chips = mesh.shape["node"], mesh.shape["expert"] // CORES
    tok_spec = P(("data", "node", "expert"), None)
    weight_spec = P(("node", "expert"), None, None)

    def local_layer(tokens, expert_ids, gate_weights, slot_ids, w_gate, w_up, w_down):
        rows, width = tokens.shape
        ff = w_gate.shape[2]
        cap = capacity(rows, expert_ids.shape[1], nodes * chips * CORES * w_gate.shape[0])
        plan = Plan(nodes, chips, cap)
        n_msgs, n_pieces = len(plan.msgs), len(plan.pieces)
        vmem, hbm = pl.BlockSpec(memory_space=pltpu.VMEM), pl.BlockSpec(memory_space=pl.ANY)
        bf16 = jnp.bfloat16
        sem = lambda n: pltpu.SemaphoreType.DMA((n,))
        parts = pl.pallas_call(
            functools.partial(kernel, plan),
            out_shape=[pltpu.VMEM((rows, width), jnp.float32), pltpu.VMEM((rows, LANES), bf16), pltpu.VMEM((LANES, width), bf16),
                       pltpu.VMEM((rows, LANES), jnp.float32)],
            in_specs=[hbm] * 7,
            out_specs=[vmem] * 4,
            scratch_shapes=[
                pltpu.VMEM((1, rows), jnp.int32),
                pltpu.VMEM((1, rows), jnp.int32),
                pltpu.VMEM((1, rows), jnp.float32),
                pltpu.VMEM((rows, width), bf16),
                pltpu.VMEM((width, ff), bf16),
                pltpu.VMEM((width, ff), bf16),
                pltpu.VMEM((ff, width), bf16),
                pltpu.VMEM((plan.rows, width), bf16),
                pltpu.VMEM((n_pieces * plan.half, width), bf16),
                pltpu.VMEM((plan.rows, width), bf16),
                pltpu.VMEM((GROUP_ROWS, ff), bf16),
                pltpu.VMEM((plan.rows, width), bf16),
                pltpu.VMEM((n_pieces * plan.half, width), bf16),
                pltpu.VMEM((plan.rows, width), bf16),
                pltpu.VMEM((rows, LANES), jnp.int32),
                sem(4), sem(3), sem(6), sem(n_msgs // 2), sem(plan.rows // GROUP_ROWS), pltpu.SemaphoreType.DMA, sem(5), sem(3),
            ],
            compiler_params=pltpu.CompilerParams(collective_id=0, has_side_effects=True, vmem_limit_bytes=VMEM_MIB * 1024 * 1024),
            name="moe_exchange",
        )(expert_ids.reshape(1, rows), slot_ids.reshape(1, rows), gate_weights.reshape(1, rows), tokens, w_gate, w_up, w_down)
        return pl.pallas_call(
            finish,
            out_shape=jax.ShapeDtypeStruct((rows, width), bf16),
            in_specs=[vmem] * 4,
            out_specs=hbm,
            scratch_shapes=[pltpu.VMEM((rows, width), bf16), pltpu.SemaphoreType.DMA],
            compiler_params=pltpu.CompilerParams(vmem_limit_bytes=8 * 1024 * 1024),
            name="moe_finish",
        )(*parts)

    return jax.shard_map(local_layer, mesh=mesh, in_specs=(tok_spec, tok_spec, tok_spec, tok_spec, weight_spec, weight_spec, weight_spec), out_specs=tok_spec, check_vma=False)
```

```python
import functools

import jax
import jax.numpy as jnp
from jax import lax
from jax.experimental import pallas as pl
from jax.experimental.pallas import tpu as pltpu
from jax.sharding import PartitionSpec as P

MESH = pl.DeviceIdType.MESH
CAP_FACTOR = 2
CORES = 2
LANES = 128
GROUP_ROWS = 256
PICK_MSGS = 2
VMEM_MIB = 52
OUT_CHUNKS = 8
X, Y = 0, 1


def capacity(rows, top_k, experts):
    return ((CAP_FACTOR * rows * top_k + 8 * experts - 1) // (8 * experts)) * 8


def far_first(n):
    return sorted(range(1, n), key=lambda d: -min(d, n - d))


class Plan:
    def __init__(self, nodes, chips, cap):
        self.size = {X: chips, Y: nodes}
        self.cap, self.half = cap, cap // 2
        self.msgs = [(a, d, c) for c in range(CORES) for i in range(max(nodes, chips) - 1) for a in (X, Y)
                     for d in far_first(self.size[a])[i:i + 1]]
        self.pieces = [(m, q) for m, (a, d, c) in enumerate(self.msgs) for q in far_first(self.size[1 - a])]
        self.piece_base = (2 + len(self.msgs)) * cap
        self.rows = self.piece_base + len(self.pieces) * self.half

    def direct_rows(self, m):
        return pl.ds((2 + m) * self.cap, self.cap)

    def piece_rows(self, k):
        return pl.ds(self.piece_base + k * self.half, self.half)

    def pieces_of(self, m):
        return [k for k, (mm, _) in enumerate(self.pieces) if mm == m]

    def spans(self):
        out = [(0, self.cap, (0, 0, 0), 0), (self.cap, self.cap, (0, 0, 1), 0)]
        for m, (a, d, c) in enumerate(self.msgs):
            out.append(((2 + m) * self.cap, self.cap, (0, d, c) if a == X else (d, 0, c), 0))
        for k, (m, q) in enumerate(self.pieces):
            a, d, c = self.msgs[m]
            out.append((self.piece_base + k * self.half, self.half, (q, d, c) if a == X else (d, q, c), 0 if a == X else self.half))
        return out


def kernel(plan, ids_hbm, slots_hbm, gates_hbm, tok_hbm, wg_hbm, wu_hbm, wd_hbm, acc, hot_ref, last_ref, gate_b,
           ids_ref, slots_ref, gates_ref, tok, wg, wu, wd, send, stage, recv, hid, y, stage2, ret, pos_b,
           in_sem, w_sem, sent, r_rel, r_grp, r_rdir, r_rpc, r_ret):
    rows = tok.shape[0]
    cap, half = plan.cap, plan.half
    nodes, chips = plan.size[Y], plan.size[X]
    data, node, exp = lax.axis_index("data"), lax.axis_index("node"), lax.axis_index("expert")
    chip, core = exp // CORES, lax.rem(exp, CORES)
    n_msgs, n_pieces = len(plan.msgs), len(plan.pieces)

    def place(dn, dx, flip):
        n, x = lax.rem(node + dn % nodes, nodes), lax.rem(chip + dx % chips, chips)
        return n, x * CORES + lax.rem(core + flip, CORES)

    def hop(axis, d, flip):
        n, e = place(0, d, flip) if axis == X else place(d, 0, flip)
        return (data, n, e)

    def first_slot(offset, slot):
        n, e = place(*offset)
        return (n * (chips * CORES) + e) * cap + slot

    def remote(src, dst, s, r, to):
        return pltpu.make_async_remote_copy(src, dst, s, r, device_id=to, device_id_type=MESH)

    def relay(m):
        ks = plan.pieces_of(m)
        part = pl.ds(ks[0] * half, len(ks) * half)
        a, d, c = plan.msgs[m]
        return remote(send.at[pl.ds(plan.piece_base + ks[0] * half, len(ks) * half)], stage.at[part], sent.at[0], r_rel.at[m // 2], hop(a, d, c))

    def forward(k):
        m, q = plan.pieces[k]
        return remote(stage.at[pl.ds(k * half, half)], recv.at[plan.piece_rows(k)], sent.at[1], r_grp.at[group_of(plan.piece_base + k * half)], hop(1 - plan.msgs[m][0], q, 0))

    last = plan.rows - LANES
    cut = plan.piece_base + (n_pieces // 2 // 4 * 4) * half

    batches = [range(0, n_msgs // 2), range(n_msgs // 2, n_msgs - 3)] + [range(m, m + 1) for m in range(n_msgs - 3, n_msgs)]

    def batch_of(m):
        return next(i for i, b in enumerate(batches) if m in b)

    def ret_part(row):
        return 0 if row < cut else 1 if row < last else 2

    def arrived(ref, lo, hi, sem):
        part = ref.at[pl.ds(lo, hi - lo)]
        pltpu.make_async_copy(part, part, sem).wait()

    def group_of(row):
        return row // GROUP_ROWS

    def direct(m, src, dst, s, r, sign):
        if m < 0:
            part, to = pl.ds(cap, cap), hop(X, 0, 1)
        else:
            a, d, c = plan.msgs[m]
            part, to = plan.direct_rows(m), hop(a, sign * d, c)
        return remote(src.at[part], dst.at[part], s, r, to)

    def out_direct(m):
        return direct(m, send, recv, sent.at[0], r_grp.at[group_of((2 + m) * cap)], 1)

    def back_direct(m):
        return direct(m, y, ret, sent.at[1], r_rdir, -1)

    def back_piece(k):
        a, d, c = plan.msgs[plan.pieces[k][0]]
        return remote(y.at[plan.piece_rows(k)], stage2.at[pl.ds(k * half, half)], sent.at[2], r_rpc.at[batch_of(plan.pieces[k][0])], hop(a, -d, c))

    def back_forward(k):
        m, q = plan.pieces[k]
        return remote(stage2.at[pl.ds(k * half, half)], ret.at[plan.piece_rows(k)], sent.at[3], r_ret.at[ret_part(plan.piece_base + k * half)], hop(1 - plan.msgs[m][0], -q, 0))

    barrier = pltpu.get_barrier_semaphore()
    near = sorted(plan.msgs, key=lambda m: -min(m[1], plan.size[m[0]] - m[1])) + [(X, 0, 1)]
    for a, d, c in near:
        pl.semaphore_signal(barrier, inc=1, device_id=hop(a, d, c), device_id_type=MESH)
    in_copies = [pltpu.make_async_copy(h, v, in_sem.at[i])
                 for i, (h, v) in enumerate(((ids_hbm, ids_ref), (slots_hbm, slots_ref), (tok_hbm, tok), (gates_hbm, gates_ref)))]
    for c in in_copies:
        c.start()
    w_copies = [pltpu.make_async_copy(h.at[0], v, w_sem.at[i]) for i, (h, v) in enumerate(((wg_hbm, wg), (wu_hbm, wu), (wd_hbm, wd)))]

    for c in in_copies:
        c.wait()
    for c in w_copies:
        c.start()
    ids, slots = ids_ref[...], slots_ref[...]
    pos = jnp.where(slots >= 0, ids * cap + slots, -1)
    spans = plan.spans()

    def pick(lo, hi):
        parts = [s for s in spans if lo <= s[0] < hi]
        hot = [jnp.where(pos - first_slot(off, slot) == lax.broadcasted_iota(jnp.int32, (size, rows), 0), 1.0, 0.0).astype(jnp.bfloat16)
               for _, size, off, slot in parts]
        got = jnp.dot(jnp.concatenate(hot, axis=0), tok[...], preferred_element_type=jnp.float32).astype(jnp.bfloat16)
        if lo == 0:
            recv[pl.ds(0, cap)] = got[:cap]
        send[pl.ds(lo, hi - lo)] = got

    todo = []
    for m in range(0, n_msgs, PICK_MSGS):
        ms = list(range(m, min(m + PICK_MSGS, n_msgs)))
        ks = [k for mm in ms for k in plan.pieces_of(mm)]
        todo.append((plan.piece_base + ks[0] * half, plan.piece_base + (ks[-1] + 1) * half, [relay(mm) for mm in ms]))
    for lo in range(0, plan.piece_base, GROUP_ROWS):
        hi = min(lo + GROUP_ROWS, plan.piece_base)
        todo.append((lo, hi, [out_direct(m) for m in range(-1, n_msgs) if lo <= (2 + m) * cap < hi]))
    for i, (lo, hi, _) in enumerate(todo):
        pick(lo, hi)
        if i == 1:
            pl.semaphore_wait(barrier, len(near))
        if i >= 1:
            for c in todo[i - 1][2]:
                c.start()
    for c in todo[-1][2]:
        c.start()

    for b in range(rows // LANES):
        pos_b[pl.ds(b * LANES, LANES), :] = jnp.transpose(jnp.broadcast_to(pos[:, b * LANES:(b + 1) * LANES], (LANES, LANES)))
        gate_b[pl.ds(b * LANES, LANES), :] = jnp.transpose(jnp.broadcast_to(gates_ref[:, b * LANES:(b + 1) * LANES], (LANES, LANES)))

    for i in range(n_msgs // 2):
        ks = plan.pieces_of(2 * i) + plan.pieces_of(2 * i + 1)
        arrived(stage, ks[0] * half, (ks[-1] + 1) * half, r_rel.at[i])
        for k in ks:
            forward(k).start()
    for c in w_copies:
        c.wait()

    n_groups = plan.rows // GROUP_ROWS

    def in_group(g):
        lo, hi = g * GROUP_ROWS, (g + 1) * GROUP_ROWS
        ms = [m for m in range(-1, n_msgs) if lo <= (2 + m) * cap < hi]
        ks = [k for k in range(n_pieces) if lo <= plan.piece_base + k * half < hi]
        return ms, ks

    def expert_group(g, carry):
        for j in range(n_groups):
            @pl.when(g == j)
            def _(j=j):
                arrived(recv, max(j * GROUP_ROWS, cap), (j + 1) * GROUP_ROWS, r_grp.at[j])
        at = pl.ds(pl.multiple_of(g * GROUP_ROWS, GROUP_ROWS), GROUP_ROWS)
        a = jnp.dot(recv[at], wg[...], preferred_element_type=jnp.float32)
        b = jnp.dot(recv[at], wu[...], preferred_element_type=jnp.float32)
        hid[...] = (jax.nn.silu(a) * b).astype(jnp.bfloat16)
        rounded = jnp.dot(hid[...], wd[...], preferred_element_type=jnp.float32).astype(jnp.bfloat16).astype(jnp.float32)
        y[at] = jnp.where(jnp.abs(rounded) < jnp.inf, rounded, 0.0).astype(jnp.bfloat16)
        for j in range(n_groups):
            @pl.when(g == j)
            def _(j=j):
                ms, ks = in_group(j)
                for m in ms:
                    back_direct(m).start()
                for k in ks:
                    back_piece(k).start()
        return carry

    lax.fori_loop(0, n_groups, expert_group, 0)
    ret[pl.ds(0, cap)] = y[pl.ds(0, cap)]

    lane = lax.broadcasted_iota(jnp.int32, (1, LANES), 1)

    def hot_rows(lo, hi):
        hots = []
        for at in range(lo, hi, LANES):
            want = None
            for first, size, off, slot in spans:
                if at <= first < at + LANES:
                    here = lane - (first - at) + first_slot(off, slot)
                    want = here if want is None else jnp.where(lane >= first - at, here, want)
            hots.append(jnp.where(pos_b[...] == want, 1.0, 0.0).astype(jnp.bfloat16))
        return jnp.concatenate(hots, axis=1) if len(hots) > 1 else hots[0]

    def picked(lo, hi):
        return jnp.dot(hot_rows(lo, hi), ret[pl.ds(lo, hi - lo)], preferred_element_type=jnp.float32)

    def send_back(ids):
        for i in ids:
            ks = [k for m in batches[i] for k in plan.pieces_of(m)]
            arrived(stage2, ks[0] * half, (ks[-1] + 1) * half, r_rpc.at[i])
            for k in ks:
                back_forward(k).start()

    send_back([0])
    arrived(ret, cap, plan.piece_base, r_rdir)
    acc[...] = picked(0, plan.piece_base)
    send_back(range(1, len(batches)))
    hot_ref[...] = hot_rows(last, plan.rows)
    for lo, hi in ((plan.piece_base, cut), (cut, last)):
        arrived(ret, lo, hi, r_ret.at[ret_part(lo)])
        acc[...] += picked(lo, hi)
    arrived(ret, last, plan.rows, r_ret.at[2])
    last_ref[...] = ret[pl.ds(last, LANES)]

    n_rows = plan.rows - plan.piece_base
    d_rows = plan.piece_base - cap
    for i, n in enumerate((n_rows + d_rows, n_rows + d_rows, n_rows, n_rows)):
        arrived(send, 0, n, sent.at[i])


def finish(acc, hot, last, gate, out_hbm, buf, sem):
    rows, width = acc.shape
    step = rows // OUT_CHUNKS
    for i in range(OUT_CHUNKS):
        at = pl.ds(i * step, step)
        total = acc[at] + jnp.dot(hot[at], last[...], preferred_element_type=jnp.float32)
        for j in range(width // LANES):
            buf[at, j * LANES:(j + 1) * LANES] = (gate[at] * total[:, j * LANES:(j + 1) * LANES]).astype(buf.dtype)
        pltpu.make_async_copy(buf.at[at], out_hbm.at[at], sem).start()
    pltpu.make_async_copy(buf, out_hbm, sem).wait()


def solution(mesh):
    nodes, chips = mesh.shape["node"], mesh.shape["expert"] // CORES
    tok_spec = P(("data", "node", "expert"), None)
    weight_spec = P(("node", "expert"), None, None)

    def local_layer(tokens, expert_ids, gate_weights, slot_ids, w_gate, w_up, w_down):
        rows, width = tokens.shape
        ff = w_gate.shape[2]
        cap = capacity(rows, expert_ids.shape[1], nodes * chips * CORES * w_gate.shape[0])
        plan = Plan(nodes, chips, cap)
        n_msgs, n_pieces = len(plan.msgs), len(plan.pieces)
        vmem, hbm = pl.BlockSpec(memory_space=pltpu.VMEM), pl.BlockSpec(memory_space=pl.ANY)
        bf16 = jnp.bfloat16
        sem = lambda n: pltpu.SemaphoreType.DMA((n,))
        parts = pl.pallas_call(
            functools.partial(kernel, plan),
            out_shape=[pltpu.VMEM((rows, width), jnp.float32), pltpu.VMEM((rows, LANES), bf16), pltpu.VMEM((LANES, width), bf16),
                       pltpu.VMEM((rows, LANES), jnp.float32)],
            in_specs=[hbm] * 7,
            out_specs=[vmem] * 4,
            scratch_shapes=[
                pltpu.VMEM((1, rows), jnp.int32),
                pltpu.VMEM((1, rows), jnp.int32),
                pltpu.VMEM((1, rows), jnp.float32),
                pltpu.VMEM((rows, width), bf16),
                pltpu.VMEM((width, ff), bf16),
                pltpu.VMEM((width, ff), bf16),
                pltpu.VMEM((ff, width), bf16),
                pltpu.VMEM((plan.rows, width), bf16),
                pltpu.VMEM((n_pieces * plan.half, width), bf16),
                pltpu.VMEM((plan.rows, width), bf16),
                pltpu.VMEM((GROUP_ROWS, ff), bf16),
                pltpu.VMEM((plan.rows, width), bf16),
                pltpu.VMEM((n_pieces * plan.half, width), bf16),
                pltpu.VMEM((plan.rows, width), bf16),
                pltpu.VMEM((rows, LANES), jnp.int32),
                sem(4), sem(3), sem(4), sem(n_msgs // 2), sem(plan.rows // GROUP_ROWS), pltpu.SemaphoreType.DMA, sem(5), sem(3),
            ],
            compiler_params=pltpu.CompilerParams(collective_id=0, has_side_effects=True, vmem_limit_bytes=VMEM_MIB * 1024 * 1024),
            name="moe_exchange",
        )(expert_ids.reshape(1, rows), slot_ids.reshape(1, rows), gate_weights.reshape(1, rows), tokens, w_gate, w_up, w_down)
        return pl.pallas_call(
            finish,
            out_shape=jax.ShapeDtypeStruct((rows, width), bf16),
            in_specs=[vmem] * 4,
            out_specs=hbm,
            scratch_shapes=[pltpu.VMEM((rows, width), bf16), pltpu.SemaphoreType.DMA],
            compiler_params=pltpu.CompilerParams(vmem_limit_bytes=8 * 1024 * 1024),
            name="moe_finish",
        )(*parts)

    return jax.shard_map(local_layer, mesh=mesh, in_specs=(tok_spec, tok_spec, tok_spec, tok_spec, weight_spec, weight_spec, weight_spec), out_specs=tok_spec, check_vma=False)
```
